32 devices in a mesh: row: 4 (over z), col: 8 (over y, x, core).
Axes of the slice: x: 2, y: 2, z: 4, core: 2. Of those that a mesh axis runs over, the one named last changes fastest.
Arguments:
- layer_input: bfloat16 [256, 8192], P('col', 'row'), may hold values from -6 to 6
- out_grad: bfloat16 [256, 8192], P('col', 'row'), may hold values from -6 to 6
- gate_weight: bfloat16 [8192, 28672], P('row', 'col'), may hold values from -0.0625 to 0.0625
- up_weight: bfloat16 [8192, 28672], P('row', 'col'), may hold values from -0.0625 to 0.0625
- down_weight: bfloat16 [28672, 8192], P('col', 'row'), may hold values from -0.03125 to 0.03125
Outputs:
- input_grad: bfloat16 [256, 8192], P('col', 'row')
- down_grad: bfloat16 [28672, 8192], P('col', 'row')
The draws below stay inside these ranges and needn't reach their ends.
All inputs are finite; a program needn't handle non-finite values.
Results may differ from the reference program's by a relative error of at most 0.0049.
Values may be sent and summed in bfloat16 or wider, within the bound.
No kernel may reach another device: no remote copies, remote signals or barrier semaphores. Data moves between devices by JAX's collectives and lax.ppermute only.
A program may use at most 128 MiB of HBM per device.

```python
import jax
import jax.numpy as jnp
from jax import lax

D = 8192
FF = 28672
TOKENS = 256


def levels(rng, dims, shards, low, top_value):
    def one(axis_at, blocks):
        draws = jax.random.uniform(jax.random.fold_in(jax.random.fold_in(rng, 6), axis_at), (blocks,), jnp.float32, low / len(shards), top_value / len(shards))
        return jnp.repeat(jnp.exp(draws), dims[axis_at] // blocks).reshape((-1,) + (1,) * (len(dims) - axis_at - 1))

    loudness = one(*shards[0])
    for cut in shards[1:]:
        loudness = loudness * one(*cut)
    return loudness


def bell_draw(rng, shape, spread, reach, cuts=(), kind=jnp.bfloat16):
    values = jax.random.normal(rng, shape, jnp.float32) * spread
    if len(cuts) > 0:
        values = levels(rng, shape, cuts, -0.22, 0.18) * values
    return jnp.clip(values, min=-reach, max=reach).astype(kind)


def setup_inputs(seed: int = 0) -> dict:
    seeds = jax.random.split(jax.random.key(seed), 6)
    layer_input = bell_draw(seeds[0], (TOKENS, D), 1.0, 6.0, ((0, 8), (1, 4)))
    out_grad = bell_draw(seeds[1], (TOKENS, D), 1.0, 6.0, ((0, 8), (1, 4)))
    gate_weight = bell_draw(seeds[2], (D, FF), D ** -0.5, 0.0625, ((0, 4), (1, 8)))
    up_weight = bell_draw(seeds[3], (D, FF), D ** -0.5, 0.0625, ((0, 4), (1, 8)))
    down_weight = bell_draw(seeds[4], (FF, D), FF ** -0.5, 0.03125, ((0, 8), (1, 4)))
    return {"layer_input": layer_input, "out_grad": out_grad, "gate_weight": gate_weight, "up_weight": up_weight, "down_weight": down_weight}


def reference(layer_input, out_grad, gate_weight, up_weight, down_weight):
    gate = jnp.dot(layer_input, gate_weight, preferred_element_type=jnp.float32)
    up = jnp.dot(layer_input, up_weight, preferred_element_type=jnp.float32)
    hidden_grad = lax.dot_general(out_grad, down_weight, (((1,), (1,)), ((), ())), preferred_element_type=jnp.float32)
    sig = jax.nn.sigmoid(gate)
    silu = gate * sig
    hidden = (silu * up).astype(jnp.bfloat16)
    up_grad = (hidden_grad * silu).astype(jnp.bfloat16)
    gate_grad = (hidden_grad * up * sig * (1.0 + gate * (1.0 - sig))).astype(jnp.bfloat16)
    down_grad = lax.dot_general(hidden, out_grad, (((0,), (0,)), ((), ())), preferred_element_type=jnp.float32).astype(jnp.bfloat16)
    first = lax.dot_general(gate_grad, gate_weight, (((1,), (1,)), ((), ())), preferred_element_type=jnp.float32)
    second = lax.dot_general(up_grad, up_weight, (((1,), (1,)), ((), ())), preferred_element_type=jnp.float32)
    input_grad = (first + second).astype(jnp.bfloat16)
    return input_grad, down_grad
```

```python
import functools

import jax
import jax.numpy as jnp
from jax import lax
from jax.experimental import pallas as pl
from jax.experimental.pallas import tpu as pltpu
from jax.sharding import PartitionSpec as P


F32, BF16 = jnp.float32, jnp.bfloat16
LANES = 128
CHUNKS = 7
GRANT = 40 * 2**20
USE_GRANT = 40 * 2**20
ACT_GRANT = 16 * 2**20


def dot(left, right, dims):
    return lax.dot_general(left, right, (dims, ((), ())), preferred_element_type=F32)


ROWS_COLS = ((1,), (0,))
LAST_LAST = ((1,), (1,))
FIRST_FIRST = ((0,), (0,))


def chunk_widths(width, count):
    unit = LANES if width % LANES == 0 else 1
    each, more = divmod(width // unit, count)
    return [unit * (each + (i < more)) for i in range(count)]


def tile_of(start, width):
    for tile in (512, 384, 256, LANES):
        if width % tile == 0 and start % tile == 0 and tile <= 512:
            if tile < width or width <= 256:
                return tile
    return LANES


def partial_kernel(*refs, sides):
    count = len(sides)
    acts, weights, part_ref, sent_ref = refs[:count], refs[count : 2 * count], refs[-2], refs[-1]
    for i, side in enumerate(sides):
        value = dot(acts[i][...], weights[i][...], side)
        part_ref[i] = value
        sent_ref[i] = value.astype(BF16)


def partials(work, start, width):
    count, depth = work[0][0].shape
    tile = tile_of(start, width)
    first = start // tile
    out = pl.BlockSpec((len(work), count, tile), lambda i: (0, 0, i))
    keep = pl.BlockSpec((count, depth), lambda i: (0, 0))
    by_column = pl.BlockSpec((depth, tile), lambda i: (0, first + i))
    by_row = pl.BlockSpec((tile, depth), lambda i: (first + i, 0))
    sides = tuple(side for _, _, side in work)
    shape = (len(work), count, width)
    return pl.pallas_call(
        functools.partial(partial_kernel, sides=sides),
        grid=(width // tile,),
        in_specs=[keep] * len(work) + [by_column if side == ROWS_COLS else by_row for side in sides],
        out_specs=[out, out],
        out_shape=[jax.ShapeDtypeStruct(shape, F32), jax.ShapeDtypeStruct(shape, BF16)],
        compiler_params=pltpu.CompilerParams(vmem_limit_bytes=GRANT),
        cost_estimate=pl.CostEstimate(
            flops=2 * len(work) * count * depth * width,
            bytes_accessed=2 * len(work) * depth * width,
            transcendentals=0,
        ),
    )(*[act for act, _, _ in work], *[weight for _, weight, _ in work])


def swiglu_kernel(*refs, shapes):
    out_ref, refs = refs[-1], list(refs[:-1])
    planes = [None, None, None]
    for stack in shapes:
        at = 0
        for size in stack:
            ref = refs.pop(0)
            for i in range(size):
                value = ref[i].astype(F32)
                planes[at] = value if planes[at] is None else planes[at] + value
                at += 1
    gate, up, hidden_grad = planes
    sig = jax.nn.sigmoid(gate)
    silu = gate * sig
    out_ref[0] = (silu * up).astype(BF16)
    out_ref[1] = (hidden_grad * up * sig * (1.0 + gate * (1.0 - sig))).astype(BF16)
    out_ref[2] = (hidden_grad * silu).astype(BF16)


def swiglu(stacks):
    _, count, width = stacks[0][0].shape
    rows = min(count, 64)
    block = lambda size: pl.BlockSpec((size, rows, width), lambda i: (0, i, 0))
    arrays = [array for stack in stacks for array in stack]
    return pl.pallas_call(
        functools.partial(swiglu_kernel, shapes=[[a.shape[0] for a in stack] for stack in stacks]),
        grid=(count // rows,),
        in_specs=[block(a.shape[0]) for a in arrays],
        out_specs=block(3),
        out_shape=jax.ShapeDtypeStruct((3, count, width), BF16),
        compiler_params=pltpu.CompilerParams(vmem_limit_bytes=ACT_GRANT),
        cost_estimate=pl.CostEstimate(
            flops=60 * count * width, bytes_accessed=30 * count * width, transcendentals=3 * count * width
        ),
    )(*arrays)


def use_kernel(pick_ref, own_ref, came_ref, g_ref, wg_ref, wu_ref, *refs, later):
    sum_ref, down_ref, done_ref = refs[-3:]

    @pl.when(pl.program_id(0) == 0)
    def _():
        came = pick_ref[0] > 0

        @pl.when(came)
        def _():
            done_ref[...] = came_ref[...]

        @pl.when(jnp.logical_not(came))
        def _():
            done_ref[...] = own_ref[...]

    total = dot(done_ref[1], wg_ref[...], LAST_LAST) + dot(done_ref[2], wu_ref[...], LAST_LAST)
    sum_ref[...] = refs[0][...] + total if later else total
    down_ref[...] = dot(done_ref[0], g_ref[...], FIRST_FIRST).astype(BF16)


def use(pick, own, came, grads, wg, wu, start, before):
    _, count, width = own.shape
    depth = grads.shape[1]
    tile = next(t for t in (512, 256, 128, depth) if depth % t == 0)
    at = start // width
    whole = pl.BlockSpec((3, count, width), lambda j: (0, 0, 0))
    columns = pl.BlockSpec((count, tile), lambda j: (0, j))
    weight = pl.BlockSpec((tile, width), lambda j: (j, at))
    operands = [pick, own, came, grads, wg, wu]
    specs = [pl.BlockSpec(memory_space=pltpu.SMEM), whole, whole, columns, weight, weight]
    if before:
        operands += before
        specs += [columns, pl.BlockSpec(memory_space=pl.ANY)]
    return pl.pallas_call(
        functools.partial(use_kernel, later=bool(before)),
        grid=(depth // tile,),
        in_specs=specs,
        out_specs=[columns, pl.BlockSpec((width, tile), lambda j: (at, j))],
        out_shape=[
            jax.ShapeDtypeStruct((count, depth), F32),
            jax.ShapeDtypeStruct((wg.shape[1], depth), BF16),
        ],
        scratch_shapes=[pltpu.VMEM((3, count, width), BF16)],
        input_output_aliases={6: 0, 7: 1} if before else {},
        compiler_params=pltpu.CompilerParams(vmem_limit_bytes=USE_GRANT),
        cost_estimate=pl.CostEstimate(
            flops=6 * count * depth * width, bytes_accessed=6 * depth * width, transcendentals=0
        ),
    )(*operands)


def near(n, i, k):
    if n & (n - 1) == 0:
        return i ^ k
    if n % 2 == 0:
        return ((i // 2 + k // 2) % (n // 2)) * 2 + (i + k) % 2
    return (i + k) % n


def fetch(x, n, k):
    return lax.ppermute(x, "col", [(near(n, i, k), i) for i in range(n)])


def give(x, n, k):
    return lax.ppermute(x, "col", [(i, near(n, i, k)) for i in range(n)])


def far_steps(n):
    return list(range(2, n, 2)) if n % 2 == 0 else list(range(1, n))


def gather_rows(x, n):
    far = [fetch(x, n, k) for k in far_steps(n)]
    mine = jnp.concatenate([x] + far)
    if n % 2 == 0:
        other = fetch(mine, n, 1)
        mine = jnp.concatenate([mine, other])
    return mine


def scatter_sum(x, n):
    if n % 2 == 0:
        near_half, far_half = jnp.split(x, 2)
        x = near_half + give(far_half, n, 1)
    steps = far_steps(n)
    blocks = jnp.split(x, 1 + len(steps))
    total = blocks[0]
    for block, k in zip(blocks[1:], steps):
        total = total + give(block.astype(BF16), n, k).astype(F32)
    return total.astype(BF16)


def make_body(n_row, n_col):
    half = n_row // 2
    inward = [[(k, k + 1), (n_row - 1 - k, n_row - 2 - k)] for k in range(half - 1)]
    across = [(half - 1, half), (half, half - 1)]
    outward = [[(b, a) for a, b in pairs] for pairs in reversed(inward)]
    steps = inward + [across]

    def body(layer_input, out_grad, gate_weight, up_weight, down_weight):
        width = gate_weight.shape[1]
        row = lax.axis_index("row")
        tokens = gather_rows(layer_input, n_col)
        grads = gather_rows(out_grad, n_col)
        before, start = None, 0
        for c, wide in enumerate(chunk_widths(width, CHUNKS)):
            work = [
                (tokens, gate_weight, ROWS_COLS),
                (tokens, up_weight, ROWS_COLS),
                (grads, down_weight, LAST_LAST),
            ]
            groups = [work[:2], work[2:]] if c == 0 else [work]
            stacks, hops = [[]], [[]]
            for group in groups:
                part, sent = partials(group, start, wide)
                hops[0].append(lax.ppermute(sent, "row", steps[0]))
                stacks[0].append(part)
            for k, pairs in enumerate(steps[1:], 1):
                sent = jnp.concatenate(stacks[0])
                for other in hops:
                    sent = sent + jnp.concatenate(other).astype(F32)
                sent = sent.astype(BF16)
                hops.append([lax.ppermute(sent, "row", pairs)])
            done = swiglu(stacks + hops)
            own, got, pick = done, done, jnp.zeros((1,), jnp.int32)
            for k, pairs in enumerate(outward):
                if k:
                    own = jnp.where(pick > 0, got, own)
                got = lax.ppermute(own, "row", pairs)
                here = jnp.logical_or(row == pairs[0][1], row == pairs[1][1])
                pick = here.astype(jnp.int32)[None]
            before = use(pick, own, got, grads, gate_weight, up_weight, start, before)
            start += wide
        return scatter_sum(before[0], n_col), before[1]

    return body


def solution(mesh):
    n_row, n_col = mesh.shape["row"], mesh.shape["col"]
    inner = make_body(n_row, n_col)

    return jax.shard_map(
        inner,
        mesh=mesh,
        in_specs=(P("col", "row"), P("col", "row"), P("row", "col"), P("row", "col"), P("col", "row")),
        out_specs=(P("col", "row"), P("col", "row")),
        check_vma=False,
    )
```
